256 devices in a mesh: owner: 8 (over y, core), rows: 32 (over z, x).
Axes of the slice: x: 4, y: 4, z: 8, core: 2. Of those that a mesh axis runs over, the one named last changes fastest.
Arguments:
- w_gate: float32 [128, 2048, 768], P('owner', 'rows'), may hold values from -0.125 to 0.125
- w_up: float32 [128, 2048, 768], P('owner', 'rows'), may hold values from -0.125 to 0.125
- router_weight: float32 [2048, 128], P('rows', 'owner'), may hold values from -0.125 to 0.125
- router_gain: float32 [2048], P('rows'), may hold values from 0.25 to 1.75
Outputs:
- serve_gate: bfloat16 [128, 768, 2048], P('owner', 'rows')
- serve_up: bfloat16 [128, 768, 2048], P('owner', 'rows')
- serve_router: bfloat16 [2048, 128], replicated
The draws below stay inside these ranges and needn't reach their ends.
All inputs are finite; a program needn't handle non-finite values.
Results may differ from the reference program's by a relative error of at most 0.001.
Values may be sent and summed in bfloat16 or wider, within the bound.
A program may use at most 64 MiB of HBM per device.

```python
import jax
import jax.numpy as jnp

EXPERTS = 128
D_MODEL = 2048
D_EXPERT = 768


def steps_of(own_key, extent, pieces, smallest, high):
    factor_of, own = 1.0, jax.random.fold_in(own_key, 6)
    for position, blocks in pieces:
        draws = jnp.exp(jax.random.uniform(jax.random.fold_in(own, position), (blocks,), jnp.float32, smallest / len(pieces), high / len(pieces)))
        factor_of = factor_of * jnp.repeat(draws, extent[position] // blocks).reshape([-1 if axis == position else 1 for axis in range(len(extent))])
    return factor_of


def gaussian(own_key, dims, spread, most, pieces=(), held_as=jnp.bfloat16):
    entries = jax.random.normal(own_key, dims, jnp.float32) * spread
    if len(pieces) > 0:
        entries = steps_of(own_key, dims, pieces, -0.22, 0.18) * entries
    return jnp.clip(entries, min=-most, max=most).astype(held_as)


def setup_inputs(seed: int = 0) -> dict:
    seeds = jax.random.split(jax.random.key(seed), 5)
    return {
        "w_gate": gaussian(seeds[0], (EXPERTS, D_MODEL, D_EXPERT), D_MODEL ** -0.5, 0.125, ((0, 8), (1, 32)), jnp.float32),
        "w_up": gaussian(seeds[1], (EXPERTS, D_MODEL, D_EXPERT), D_MODEL ** -0.5, 0.125, ((0, 8), (1, 32)), jnp.float32),
        "router_weight": gaussian(seeds[2], (D_MODEL, EXPERTS), D_MODEL ** -0.5, 0.125, ((0, 32), (1, 8)), jnp.float32),
        "router_gain": jnp.clip(1.0 + 0.15 * jax.random.normal(seeds[3], (D_MODEL,), jnp.float32), 0.25, 1.75),
    }


def reference(w_gate, w_up, router_weight, router_gain):
    serve_gate = w_gate.astype(jnp.bfloat16)
    serve_gate = jnp.transpose(serve_gate, (0, 2, 1))
    serve_up = w_up.astype(jnp.bfloat16)
    serve_up = jnp.transpose(serve_up, (0, 2, 1))
    serve_router = (router_weight * router_gain[:, None]).astype(jnp.bfloat16)
    return serve_gate, serve_up, serve_router
```

```python
import jax
import jax.numpy as jnp
from jax import lax
from jax.experimental import pallas as pl
from jax.experimental.pallas import tpu as pltpu
from jax.sharding import PartitionSpec as P

MESH = pl.DeviceIdType.MESH
NZ, NX, NY, CORES = 8, 4, 4, 2
ROWS = NZ * NX
LANES, SUB = 128, 8


def place():
    owner, rows = lax.axis_index("owner"), lax.axis_index("rows")
    return owner // CORES, lax.rem(owner, CORES), rows // NX, lax.rem(rows, NX)


def beside(value, step, count):
    return lax.rem(value + step, count)


def rows_of(k):
    _, _, z, x = place()
    return beside(z, k // NX, NZ) * NX + beside(x, lax.rem(k, NX), NX)


def merged(even, odd):
    low = lax.broadcasted_iota(jnp.int32, even.shape, even.ndim - 1) < LANES // 2
    turned_odd = pltpu.roll(odd, LANES // 2, odd.ndim - 1)
    turned_even = pltpu.roll(even, LANES // 2, even.ndim - 1)
    return jnp.where(low, even, turned_odd), jnp.where(low, turned_even, odd)


def kernel(
    gate, up, weight, gain, out_gate, out_up, out_router,
    staged, send, recv, pieces, in_sem, send_sem, recv_sem, piece_send, piece_recv,
):
    y, core, z, x = place()
    owner, rows = lax.axis_index("owner"), lax.axis_index("rows")
    pairs = gate.shape[0]
    width = gate.shape[2]
    tiles = width // ROWS // SUB
    sources = (gate, up)

    def load(a, p):
        return pltpu.make_async_copy(sources[a].at[p], staged.at[p, a], in_sem.at[p, a])

    def load_all(p, _):
        for a in range(2):
            load(a, p).start()
        return 0

    lax.fori_loop(0, pairs, load_all, 0)

    barrier = pltpu.get_barrier_semaphore()

    def greet(k, _):
        pl.semaphore_signal(barrier, inc=1, device_id={"rows": rows_of(k)}, device_id_type=MESH)
        return 0

    lax.fori_loop(1, ROWS, greet, 0)
    y_peers = [beside(y, k, NY) * CORES + core for k in range(1, NY)]
    partner = y * CORES + (1 - core)
    for peer in (*y_peers, partner):
        pl.semaphore_signal(barrier, inc=1, device_id={"owner": peer}, device_id_type=MESH)

    scaled = weight[...] * gain[...]
    pieces[core, y, x, z] = jnp.concatenate([scaled[:SUB], scaled[SUB:]], axis=1).astype(jnp.bfloat16)

    def prepare(p):
        for a in range(2):
            load(a, p).wait()
            for k in range(width // LANES):
                block = staged[p, a, :, k * LANES : (k + 1) * LANES].T.reshape(LANES // SUB, SUB, LANES)
                block = block.astype(jnp.bfloat16)
                for i in range(LANES // SUB):
                    g = k * (LANES // SUB) + i
                    send[p, g // tiles, a * tiles + g % tiles] = block[i]
        recv[p, rows] = send[p, rows]

    def move(p, peer):
        return pltpu.make_async_remote_copy(
            send.at[p, peer], recv.at[p, rows], send_sem.at[p], recv_sem.at[p, rows],
            device_id={"rows": peer}, device_id_type=MESH,
        )

    def send_all(p):
        def one(k, _):
            move(p, rows_of(k)).start()
            return 0

        lax.fori_loop(1, ROWS, one, 0)

    def arrived(p, source):
        pltpu.make_async_remote_copy(
            send.at[p, source], recv.at[p, source], send_sem.at[p], recv_sem.at[p, source],
            device_id={"rows": rows}, device_id_type=MESH,
        ).wait_recv()

    def assemble(p):
        def pair(j, _):
            for s in (2 * j, 2 * j + 1):
                @pl.when(s != rows)
                def _():
                    arrived(p, s)

            low, high = merged(recv[p, 2 * j], recv[p, 2 * j + 1])
            lanes = pl.ds(pl.multiple_of(j * LANES, LANES), LANES)
            for a, out in enumerate((out_gate, out_up)):
                out[2 * p, :, :, lanes] = low[a * tiles : (a + 1) * tiles]
                out[2 * p + 1, :, :, lanes] = high[a * tiles : (a + 1) * tiles]
            return 0

        lax.fori_loop(0, ROWS // 2, pair, 0)

    def to_z(k):
        mine = pieces.at[core, y, x, z]
        return pltpu.make_async_remote_copy(
            mine, mine, piece_send.at[0, k], piece_recv.at[0, k],
            device_id={"rows": beside(z, k, NZ) * NX + x}, device_id_type=MESH,
        )

    def to_x(k):
        mine = pieces.at[core, y, x]
        return pltpu.make_async_remote_copy(
            mine, mine, piece_send.at[1, k], piece_recv.at[1, k],
            device_id={"rows": z * NX + beside(x, k, NX)}, device_id_type=MESH,
        )

    def to_y(k):
        mine = pieces.at[core, y]
        return pltpu.make_async_remote_copy(
            mine, mine, piece_send.at[2, k], piece_recv.at[2, k],
            device_id={"owner": beside(y, k, NY) * CORES + core}, device_id_type=MESH,
        )

    def to_core(k):
        mine = pieces.at[core]
        return pltpu.make_async_remote_copy(
            mine, mine, piece_send.at[3, k], piece_recv.at[3, k],
            device_id={"owner": partner}, device_id_type=MESH,
        )

    stages = ((to_z, NZ), (to_x, NX), (to_y, NY), (to_core, CORES))

    def begin(stage):
        to, count = stages[stage]
        for k in range(1, count):
            to(k).start()

    def end(stage):
        to, count = stages[stage]
        for k in range(1, count):
            to(k).wait()

    def router():
        for zz in range(NZ):
            for half in range(NX // 2):
                blocks = []
                for o in range(NY * CORES):
                    low, high = merged(
                        pieces[o % CORES, o // CORES, 2 * half, zz], pieces[o % CORES, o // CORES, 2 * half + 1, zz]
                    )
                    blocks += [low, high]
                block = jnp.concatenate([b.astype(jnp.float32) for b in blocks], axis=0)
                at = (zz * NX + 2 * half) * LANES // 2
                out_router[at : at + LANES, :] = block.T.astype(jnp.bfloat16)

    prepare(0)
    pl.semaphore_wait(barrier, ROWS - 1 + NY)
    begin(0)
    send_all(0)
    prepare(1)
    send_all(1)
    end(0)
    begin(1)
    for p in (2, 3):
        prepare(p)
        send_all(p)
    end(1)
    begin(2)

    def rest(p, _):
        prepare(p)
        send_all(p)
        return 0

    lax.fori_loop(4, pairs, rest, 0)
    assemble(0)
    end(2)
    begin(3)
    assemble(1)
    end(3)
    router()

    def finish(p, _):
        assemble(p)
        return 0

    lax.fori_loop(2, pairs, finish, 0)

    def sent(p, _):
        others = pl.ds(0, ROWS - 1)
        pltpu.make_async_remote_copy(
            send.at[p, others], recv.at[p, others], send_sem.at[p], recv_sem.at[p, 0],
            device_id={"rows": rows}, device_id_type=MESH,
        ).wait_send()
        return 0

    lax.fori_loop(0, pairs, sent, 0)


def body(w_gate, w_up, router_weight, router_gain):
    experts, share, width = w_gate.shape
    pairs, model = experts // 2, share * ROWS
    tiles = width // ROWS // SUB
    paired = (pairs, 2 * share, width)
    vmem, anywhere = pl.BlockSpec(memory_space=pltpu.VMEM), pl.BlockSpec(memory_space=pl.ANY)
    gate, up, router = pl.pallas_call(
        kernel,
        out_shape=(
            jax.ShapeDtypeStruct((experts, tiles, SUB, model), jnp.bfloat16),
            jax.ShapeDtypeStruct((experts, tiles, SUB, model), jnp.bfloat16),
            jax.ShapeDtypeStruct((model, experts * NY * CORES), jnp.bfloat16),
        ),
        in_specs=[anywhere, anywhere, vmem, vmem],
        out_specs=(vmem, vmem, vmem),
        scratch_shapes=[
            pltpu.VMEM((pairs, 2, 2 * share, width), jnp.float32),
            pltpu.VMEM((pairs, ROWS, 2 * tiles, SUB, LANES), jnp.bfloat16),
            pltpu.VMEM((pairs, ROWS, 2 * tiles, SUB, LANES), jnp.bfloat16),
            pltpu.VMEM((CORES, NY, NX, NZ, SUB, LANES), jnp.bfloat16),
            pltpu.SemaphoreType.DMA((pairs, 2)),
            pltpu.SemaphoreType.DMA((pairs,)),
            pltpu.SemaphoreType.DMA((pairs, ROWS)),
            pltpu.SemaphoreType.DMA((4, NZ)),
            pltpu.SemaphoreType.DMA((4, NZ)),
        ],
        compiler_params=pltpu.CompilerParams(collective_id=0, has_side_effects=True, vmem_limit_bytes=50000000),
        name="serve",
    )(w_gate.reshape(paired), w_up.reshape(paired), router_weight.T, router_gain.reshape(1, share))
    shape = (experts, tiles * SUB, model)
    return gate.reshape(shape), up.reshape(shape), router


def solution(mesh):
    return jax.shard_map(
        body,
        mesh=mesh,
        in_specs=(P("owner", "rows", None), P("owner", "rows", None), P("rows", "owner"), P("rows")),
        out_specs=(P("owner", "rows", None), P("owner", "rows", None), P()),
        check_vma=False,
    )
```

```python
import jax
import jax.numpy as jnp
from jax import lax
from jax.experimental import pallas as pl
from jax.experimental.pallas import tpu as pltpu
from jax.sharding import PartitionSpec as P

MESH = pl.DeviceIdType.MESH
NZ, NX, NY, CORES = 8, 4, 4, 2
ROWS = NZ * NX
LANES, SUB = 128, 8
TOGETHER = 8
PARTS = 4


def place():
    owner, rows = lax.axis_index("owner"), lax.axis_index("rows")
    return owner // CORES, lax.rem(owner, CORES), rows // NX, lax.rem(rows, NX)


def beside(value, step, count):
    return lax.rem(value + step, count)


def rows_of(k):
    _, _, z, x = place()
    return beside(z, lax.rem(k, NZ), NZ) * NX + beside(x, k // NZ, NX)


def merged(even, odd):
    low = lax.broadcasted_iota(jnp.int32, even.shape, even.ndim - 1) < LANES // 2
    turned = pltpu.roll(jnp.where(low, odd, even), LANES // 2, even.ndim - 1)
    return jnp.where(low, even, turned), jnp.where(low, turned, odd)


def kernel(
    gate, up, weight, out_gate, out_up, out_router,
    staged, send, recv, pieces, in_sem, send_sem, recv_sem, piece_send, piece_recv,
):
    y, core, z, x = place()
    owner, rows = lax.axis_index("owner"), lax.axis_index("rows")
    pairs = gate.shape[0]
    width = gate.shape[2]
    tiles = width // ROWS // SUB
    sources = (gate, up)

    def load(a, p):
        return pltpu.make_async_copy(sources[a].at[p], staged.at[p, a], in_sem.at[p, a])

    def load_all(p, _):
        for a in range(2):
            load(a, p).start()
        return 0

    lax.fori_loop(0, pairs, load_all, 0)

    barrier = pltpu.get_barrier_semaphore()

    def greet(k, _):
        pl.semaphore_signal(barrier, inc=1, device_id={"rows": rows_of(k)}, device_id_type=MESH)
        return 0

    lax.fori_loop(1, ROWS, greet, 0)
    y_peers = [beside(y, k, NY) * CORES + core for k in range(1, NY)]
    partner = y * CORES + (1 - core)
    for peer in (*y_peers, partner):
        pl.semaphore_signal(barrier, inc=1, device_id={"owner": peer}, device_id_type=MESH)

    scaled = weight[...]
    pieces[core, y, x, z] = jnp.concatenate([scaled[:SUB], scaled[SUB:]], axis=1).astype(jnp.bfloat16)

    def prepare(p):
        for a in range(2):
            load(a, p).wait()
            for k in range(width // LANES):
                block = staged[p, a, :, k * LANES : (k + 1) * LANES].T.reshape(LANES // SUB, SUB, LANES)
                block = block.astype(jnp.bfloat16)
                for i in range(LANES // SUB):
                    g = k * (LANES // SUB) + i
                    send[p, g // tiles, a * tiles + g % tiles] = block[i]
        recv[p, rows] = send[p, rows]

    def move(p, peer):
        return pltpu.make_async_remote_copy(
            send.at[p, peer], recv.at[p, rows], send_sem.at[p], recv_sem.at[p, rows],
            device_id={"rows": peer}, device_id_type=MESH,
        )

    def send_all(p):
        def one(k, _):
            move(p, rows_of(k)).start()
            return 0

        lax.fori_loop(1, ROWS, one, 0)

    def arrived(p, source):
        pltpu.make_async_remote_copy(
            send.at[p, source], recv.at[p, source], send_sem.at[p], recv_sem.at[p, source],
            device_id={"rows": rows}, device_id_type=MESH,
        ).wait_recv()

    def assemble(p):
        def some(t, _):
            for i in range(TOGETHER):
                for s in (2 * (t * TOGETHER + i), 2 * (t * TOGETHER + i) + 1):
                    @pl.when(s != rows)
                    def _():
                        arrived(p, s)

            for i in range(TOGETHER):
                j = t * TOGETHER + i
                low, high = merged(recv[p, 2 * j], recv[p, 2 * j + 1])
                lanes = pl.ds(pl.multiple_of(j * LANES, LANES), LANES)
                for a, out in enumerate((out_gate, out_up)):
                    out[2 * p, :, :, lanes] = low[a * tiles : (a + 1) * tiles]
                    out[2 * p + 1, :, :, lanes] = high[a * tiles : (a + 1) * tiles]
            return 0

        lax.fori_loop(0, ROWS // 2 // TOGETHER, some, 0)

    def to_z(k):
        mine = pieces.at[core, y, x, z]
        return pltpu.make_async_remote_copy(
            mine, mine, piece_send.at[0, k], piece_recv.at[0, k],
            device_id={"rows": beside(z, k, NZ) * NX + x}, device_id_type=MESH,
        )

    def to_x(k):
        mine = pieces.at[core, y, x]
        return pltpu.make_async_remote_copy(
            mine, mine, piece_send.at[1, k], piece_recv.at[1, k],
            device_id={"rows": z * NX + beside(x, k, NX)}, device_id_type=MESH,
        )

    def to_y(k):
        mine = pieces.at[core, y]
        return pltpu.make_async_remote_copy(
            mine, mine, piece_send.at[2, k], piece_recv.at[2, k],
            device_id={"owner": beside(y, k, NY) * CORES + core}, device_id_type=MESH,
        )

    def to_core(k):
        mine = pieces.at[core]
        return pltpu.make_async_remote_copy(
            mine, mine, piece_send.at[3, k], piece_recv.at[3, k],
            device_id={"owner": partner}, device_id_type=MESH,
        )

    stages = ((to_z, NZ), (to_x, NX), (to_y, NY), (to_core, CORES))

    def begin(stage):
        to, count = stages[stage]
        for k in range(1, count):
            to(k).start()

    def end(stage):
        to, count = stages[stage]
        for k in range(1, count):
            to(k).wait()

    def router():
        for zz in range(NZ):
            for half in range(NX // 2):
                blocks = []
                for o in range(NY * CORES):
                    low, high = merged(
                        pieces[o % CORES, o // CORES, 2 * half, zz], pieces[o % CORES, o // CORES, 2 * half + 1, zz]
                    )
                    blocks += [low, high]
                block = jnp.concatenate([b.astype(jnp.float32) for b in blocks], axis=0)
                at = (zz * NX + 2 * half) * LANES // 2
                out_router[at : at + LANES, :] = block.T.astype(jnp.bfloat16)

    prepare(0)
    pl.semaphore_wait(barrier, ROWS - 1 + NY)
    begin(0)
    send_all(0)
    prepare(1)
    send_all(1)
    end(0)
    begin(1)
    for p in (2, 3):
        prepare(p)
        send_all(p)
    end(1)
    begin(2)

    def rest(p, _):
        prepare(p)
        send_all(p)
        return 0

    lax.fori_loop(4, pairs, rest, 0)
    assemble(0)
    end(2)
    begin(3)
    assemble(1)
    end(3)
    router()

    def finish(p, _):
        assemble(p)
        return 0

    lax.fori_loop(2, pairs, finish, 0)

    def sent(p, _):
        others = pl.ds(0, ROWS - 1)
        pltpu.make_async_remote_copy(
            send.at[p, others], recv.at[p, others], send_sem.at[p], recv_sem.at[p, 0],
            device_id={"rows": rows}, device_id_type=MESH,
        ).wait_send()
        return 0

    lax.fori_loop(0, pairs, sent, 0)


def store(*refs):
    count = len(refs) // 2
    copies = []
    for k, (source, target) in enumerate(zip(refs[:count], refs[count : 2 * count])):
        step = source.shape[0] // PARTS
        for i in range(PARTS):
            part = pl.ds(i * step, step)
            copies.append(pltpu.make_async_copy(source.at[part], target.at[part], refs[-1].at[k, i]))
    for copy in copies:
        copy.start()
    for copy in copies:
        copy.wait()


def body(w_gate, w_up, router_weight, router_gain):
    experts, share, width = w_gate.shape
    pairs, model = experts // 2, share * ROWS
    tiles = width // ROWS // SUB
    paired = (pairs, 2 * share, width)
    vmem, anywhere = pl.BlockSpec(memory_space=pltpu.VMEM), pl.BlockSpec(memory_space=pl.ANY)
    gate, up, router = pl.pallas_call(
        kernel,
        out_shape=(
            jax.ShapeDtypeStruct((experts, tiles, SUB, model), jnp.bfloat16),
            jax.ShapeDtypeStruct((experts, tiles, SUB, model), jnp.bfloat16),
            jax.ShapeDtypeStruct((model, experts * NY * CORES), jnp.bfloat16),
        ),
        in_specs=[anywhere, anywhere, vmem],
        out_specs=(vmem, vmem, vmem),
        scratch_shapes=[
            pltpu.VMEM((pairs, 2, 2 * share, width), jnp.float32),
            pltpu.VMEM((pairs, ROWS, 2 * tiles, SUB, LANES), jnp.bfloat16),
            pltpu.VMEM((pairs, ROWS, 2 * tiles, SUB, LANES), jnp.bfloat16),
            pltpu.VMEM((CORES, NY, NX, NZ, SUB, LANES), jnp.bfloat16),
            pltpu.SemaphoreType.DMA((pairs, 2)),
            pltpu.SemaphoreType.DMA((pairs,)),
            pltpu.SemaphoreType.DMA((pairs, ROWS)),
            pltpu.SemaphoreType.DMA((4, NZ)),
            pltpu.SemaphoreType.DMA((4, NZ)),
        ],
        compiler_params=pltpu.CompilerParams(collective_id=0, has_side_effects=True, vmem_limit_bytes=50000000),
        name="serve",
    )(w_gate.reshape(paired), w_up.reshape(paired), (router_weight * router_gain[:, None]).T)
    gate, up, router = pl.pallas_call(
        store,
        out_shape=tuple(jax.ShapeDtypeStruct(v.shape, v.dtype) for v in (gate, up, router)),
        in_specs=[vmem] * 3,
        out_specs=(anywhere,) * 3,
        scratch_shapes=[pltpu.SemaphoreType.DMA((3, PARTS))],
        compiler_params=pltpu.CompilerParams(vmem_limit_bytes=50000000),
        name="store",
    )(gate, up, router)
    shape = (experts, tiles * SUB, model)
    return gate.reshape(shape), up.reshape(shape), router


def solution(mesh):
    return jax.shard_map(
        body,
        mesh=mesh,
        in_specs=(P("owner", "rows", None), P("owner", "rows", None), P("rows", "owner"), P("rows")),
        out_specs=(P("owner", "rows", None), P("owner", "rows", None), P()),
        check_vma=False,
    )
```

```python
import jax
import jax.numpy as jnp
from jax import lax
from jax.experimental import pallas as pl
from jax.experimental.pallas import tpu as pltpu
from jax.sharding import PartitionSpec as P

MESH = pl.DeviceIdType.MESH
NZ, NX, NY, CORES = 8, 4, 4, 2
ROWS = NZ * NX
LANES, SUB = 128, 8
TOGETHER = 8
PARTS = 4
ORDER = [(dx, dz) for dx in (2, 1, 3, 0) for dz in (4, 3, 5, 2, 6, 1, 7, 0) if dx or dz]


def place():
    owner, rows = lax.axis_index("owner"), lax.axis_index("rows")
    return owner // CORES, owner % CORES, rows // NX, rows % NX


def beside(value, step, count):
    return (value + step) % count


def merged(even, odd):
    low = lax.broadcasted_iota(jnp.int32, even.shape, even.ndim - 1) < LANES // 2
    turned = pltpu.roll(jnp.where(low, odd, even), LANES // 2, even.ndim - 1)
    return jnp.where(low, even, turned), jnp.where(low, turned, odd)


def kernel(
    gate, up, weight, out_gate, out_up, out_router,
    staged, send, recv, pieces, in_sem, send_sem, recv_sem, piece_send, piece_recv,
):
    y, core, z, x = place()
    owner, rows = lax.axis_index("owner"), lax.axis_index("rows")
    pairs = gate.shape[0]
    width = gate.shape[2]
    tiles = width // ROWS // SUB
    sources = (gate, up)

    def load(a, p):
        return pltpu.make_async_copy(sources[a].at[p], staged.at[p, a], in_sem.at[p])

    def load_all(p, _):
        for a in range(2):
            load(a, p).start()
        return 0

    lax.fori_loop(0, pairs, load_all, 0)

    barrier = pltpu.get_barrier_semaphore()

    lines = [beside(z, dz, NZ) * NX for dz in range(NZ)]
    columns = [beside(x, dx, NX) for dx in range(NX)]
    peers = [lines[dz] + columns[dx] for dx, dz in ORDER]
    for peer in peers:
        pl.semaphore_signal(barrier, inc=1, device_id={"rows": peer}, device_id_type=MESH)
    y_peers = [beside(y, k, NY) * CORES + core for k in range(1, NY)]
    partner = y * CORES + (1 - core)
    for peer in (*y_peers, partner):
        pl.semaphore_signal(barrier, inc=1, device_id={"owner": peer}, device_id_type=MESH)

    scaled = weight[...]
    pieces[core, y, x, z] = jnp.concatenate([scaled[:SUB], scaled[SUB:]], axis=1).astype(jnp.bfloat16)

    def prepare(p):
        pltpu.make_async_copy(gate.at[pl.ds(0, 2)], staged.at[p], in_sem.at[p]).wait()
        for a in range(2):
            for k in range(width // LANES):
                block = staged[p, a, :, k * LANES : (k + 1) * LANES].T.reshape(LANES // SUB, SUB, LANES)
                block = block.astype(jnp.bfloat16)
                for i in range(LANES // SUB):
                    g = k * (LANES // SUB) + i
                    send[p, g // tiles, a * tiles + g % tiles] = block[i]
        recv[p, rows] = send[p, rows]

    def move(p, peer):
        return pltpu.make_async_remote_copy(
            send.at[p, peer], recv.at[p, rows], send_sem.at[p], recv_sem.at[p],
            device_id={"rows": peer}, device_id_type=MESH,
        )

    def send_all(p):
        for peer in peers:
            move(p, peer).start()

    def all_of(p):
        others = pl.ds(0, ROWS - 1)
        return pltpu.make_async_remote_copy(
            send.at[p, others], recv.at[p, others], send_sem.at[p], recv_sem.at[p],
            device_id={"rows": rows}, device_id_type=MESH,
        )

    def assemble(p):
        all_of(p).wait_recv()

        def some(t, _):
            for i in range(TOGETHER):
                j = t * TOGETHER + i
                low, high = merged(recv[p, 2 * j], recv[p, 2 * j + 1])
                lanes = pl.ds(pl.multiple_of(j * LANES, LANES), LANES)
                for a, out in enumerate((out_gate, out_up)):
                    out[2 * p, :, :, lanes] = low[a * tiles : (a + 1) * tiles]
                    out[2 * p + 1, :, :, lanes] = high[a * tiles : (a + 1) * tiles]
            return 0

        lax.fori_loop(0, ROWS // 2 // TOGETHER, some, 0)

    def to_z(k):
        mine = pieces.at[core, y, x, z]
        return pltpu.make_async_remote_copy(
            mine, mine, piece_send.at[0], piece_recv.at[0],
            device_id={"rows": beside(z, k, NZ) * NX + x}, device_id_type=MESH,
        )

    def to_x(k):
        mine = pieces.at[core, y, x]
        return pltpu.make_async_remote_copy(
            mine, mine, piece_send.at[1], piece_recv.at[1],
            device_id={"rows": z * NX + beside(x, k, NX)}, device_id_type=MESH,
        )

    def to_y(k):
        mine = pieces.at[core, y]
        return pltpu.make_async_remote_copy(
            mine, mine, piece_send.at[2], piece_recv.at[2],
            device_id={"owner": beside(y, k, NY) * CORES + core}, device_id_type=MESH,
        )

    def to_core(k):
        mine = pieces.at[core]
        return pltpu.make_async_remote_copy(
            mine, mine, piece_send.at[3], piece_recv.at[3],
            device_id={"owner": partner}, device_id_type=MESH,
        )

    stages = ((to_z, NZ), (to_x, NX), (to_y, NY), (to_core, CORES))

    def begin(stage):
        to, count = stages[stage]
        for k in range(1, count):
            to(k).start()

    def end(stage):
        whole = (
            pieces.at[core, y, x, pl.ds(0, NZ - 1)],
            pieces.at[core, y, pl.ds(0, NX - 1)],
            pieces.at[core, pl.ds(0, NY - 1)],
            pieces.at[core],
        )[stage]
        pltpu.make_async_remote_copy(
            whole, whole, piece_send.at[stage], piece_recv.at[stage],
            device_id={"rows": rows}, device_id_type=MESH,
        ).wait()

    def router():
        for zz in range(NZ):
            for half in range(NX // 2):
                blocks = []
                for o in range(NY * CORES):
                    low, high = merged(
                        pieces[o % CORES, o // CORES, 2 * half, zz], pieces[o % CORES, o // CORES, 2 * half + 1, zz]
                    )
                    blocks += [low, high]
                block = jnp.concatenate([b.astype(jnp.float32) for b in blocks], axis=0)
                at = (zz * NX + 2 * half) * LANES // 2
                out_router[at : at + LANES, :] = block.T.astype(jnp.bfloat16)

    prepare(0)
    pl.semaphore_wait(barrier, ROWS - 1 + NY)
    begin(0)
    send_all(0)
    prepare(1)
    send_all(1)
    end(0)
    begin(1)
    for p in (2, 3):
        prepare(p)
        send_all(p)
    end(1)
    begin(2)

    def rest(p, _):
        prepare(p)
        send_all(p)
        return 0

    lax.fori_loop(4, pairs, rest, 0)
    assemble(0)
    end(2)
    begin(3)
    assemble(1)
    end(3)
    router()

    def finish(p, _):
        assemble(p)
        return 0

    lax.fori_loop(2, pairs, finish, 0)

    def sent(p, _):
        all_of(p).wait_send()
        return 0

    lax.fori_loop(0, pairs, sent, 0)


def store(*refs):
    count = len(refs) // 2
    copies = []
    for k, (source, target) in enumerate(zip(refs[:count], refs[count : 2 * count])):
        step = source.shape[0] // PARTS
        for i in range(PARTS):
            part = pl.ds(i * step, step)
            copies.append(pltpu.make_async_copy(source.at[part], target.at[part], refs[-1].at[k, i]))
    for copy in copies:
        copy.start()
    for copy in copies:
        copy.wait()


def body(w_gate, w_up, router_weight, router_gain):
    experts, share, width = w_gate.shape
    pairs, model = experts // 2, share * ROWS
    tiles = width // ROWS // SUB
    paired = (pairs, 2 * share, width)
    vmem, anywhere = pl.BlockSpec(memory_space=pltpu.VMEM), pl.BlockSpec(memory_space=pl.ANY)
    gate, up, router = pl.pallas_call(
        kernel,
        out_shape=(
            jax.ShapeDtypeStruct((experts, tiles, SUB, model), jnp.bfloat16),
            jax.ShapeDtypeStruct((experts, tiles, SUB, model), jnp.bfloat16),
            jax.ShapeDtypeStruct((model, experts * NY * CORES), jnp.bfloat16),
        ),
        in_specs=[anywhere, anywhere, vmem],
        out_specs=(vmem, vmem, vmem),
        scratch_shapes=[
            pltpu.VMEM((pairs, 2, 2 * share, width), jnp.float32),
            pltpu.VMEM((pairs, ROWS, 2 * tiles, SUB, LANES), jnp.bfloat16),
            pltpu.VMEM((pairs, ROWS, 2 * tiles, SUB, LANES), jnp.bfloat16),
            pltpu.VMEM((CORES, NY, NX, NZ, SUB, LANES), jnp.bfloat16),
            pltpu.SemaphoreType.DMA((pairs,)),
            pltpu.SemaphoreType.DMA((pairs,)),
            pltpu.SemaphoreType.DMA((pairs,)),
            pltpu.SemaphoreType.DMA((4,)),
            pltpu.SemaphoreType.DMA((4,)),
        ],
        compiler_params=pltpu.CompilerParams(collective_id=0, has_side_effects=True, vmem_limit_bytes=50000000),
        name="serve",
    )(w_gate.reshape(paired), w_up.reshape(paired), (router_weight * router_gain[:, None]).T)
    gate, up, router = pl.pallas_call(
        store,
        out_shape=tuple(jax.ShapeDtypeStruct(v.shape, v.dtype) for v in (gate, up, router)),
        in_specs=[vmem] * 3,
        out_specs=(anywhere,) * 3,
        scratch_shapes=[pltpu.SemaphoreType.DMA((3, PARTS))],
        compiler_params=pltpu.CompilerParams(vmem_limit_bytes=50000000),
        name="store",
    )(gate, up, router)
    shape = (experts, tiles * SUB, model)
    return gate.reshape(shape), up.reshape(shape), router


def solution(mesh):
    return jax.shard_map(
        body,
        mesh=mesh,
        in_specs=(P("owner", "rows", None), P("owner", "rows", None), P("rows", "owner"), P("rows")),
        out_specs=(P("owner", "rows", None), P("owner", "rows", None), P()),
        check_vma=False,
    )
```

```python
import jax
import jax.numpy as jnp
from jax import lax
from jax.experimental import pallas as pl
from jax.experimental.pallas import tpu as pltpu
from jax.sharding import PartitionSpec as P

MESH = pl.DeviceIdType.MESH
NZ, NX, NY, CORES = 8, 4, 4, 2
ROWS = NZ * NX
LANES, SUB = 128, 8
TOGETHER = 8
PARTS = 4
EARLY = 2
REACH = [
    [(0, dz) for dz in sorted({r + 1, NZ - r - 1}) if r + 1 <= NZ // 2]
    + [(dx, dz) for dz in sorted({r, (NZ - r) % NZ}) for dx in range(1, NX)]
    for r in range(NZ // 2 + 1)
]
ORDER = [(dx, dz) for dx in (2, 1, 3, 0) for dz in (4, 3, 5, 2, 6, 1, 7, 0) if dx or dz]


def place():
    owner, rows = lax.axis_index("owner"), lax.axis_index("rows")
    return owner // CORES, owner % CORES, rows // NX, rows % NX


def beside(value, step, count):
    return (value + step) % count


def merged(even, odd):
    low = lax.broadcasted_iota(jnp.int32, even.shape, even.ndim - 1) < LANES // 2
    turned = pltpu.roll(jnp.where(low, odd, even), LANES // 2, even.ndim - 1)
    return jnp.where(low, even, turned), jnp.where(low, turned, odd)


def kernel(
    gate, up, weight, gain, out_gate, out_up, out_router,
    staged, weights, gains, send, recv, pieces, in_sem, router_sem, send_sem, recv_sem, piece_send, piece_recv, rounds,
):
    y, core, z, x = place()
    owner, rows = lax.axis_index("owner"), lax.axis_index("rows")
    pairs = gate.shape[0]
    width = gate.shape[2]
    tiles = width // ROWS // SUB
    sources = (gate, up)

    def load(a, p):
        return pltpu.make_async_copy(sources[a].at[p], staged.at[p, a], in_sem.at[p])

    def load_all(p, _):
        for a in range(2):
            load(a, p).start()
        return 0

    barrier = pltpu.get_barrier_semaphore()

    lines = [beside(z, dz, NZ) * NX for dz in range(NZ)]
    columns = [beside(x, dx, NX) for dx in range(NX)]
    peers = [lines[dz] + columns[dx] for dx, dz in ORDER]
    y_peers = [beside(y, k, NY) * CORES + core for k in range(1, NY)]
    partner = y * CORES + (1 - core)
    beside_z = [lines[1] + x, lines[NZ - 1] + x]
    for peer in beside_z + [z * NX + columns[dx] for dx in range(1, NX)]:
        pl.semaphore_signal(barrier, inc=1, device_id={"rows": peer}, device_id_type=MESH)
    for peer in (*y_peers, partner):
        pl.semaphore_signal(barrier, inc=1, device_id={"owner": peer}, device_id_type=MESH)

    router_loads = (
        pltpu.make_async_copy(weight, weights, router_sem.at[0]),
        pltpu.make_async_copy(gain, gains, router_sem.at[1]),
    )
    for copy in router_loads:
        copy.start()
    lax.fori_loop(0, pairs, load_all, 0)

    for copy in router_loads:
        copy.wait()
    scaled = weights[...] * gains[...]
    pieces[core, y, x, z] = jnp.concatenate([scaled[:SUB], scaled[SUB:]], axis=1).astype(jnp.bfloat16)

    def prepare(p):
        pltpu.make_async_copy(gate.at[pl.ds(0, 2)], staged.at[p], in_sem.at[p]).wait()
        for a in range(2):
            for k in range(width // LANES):
                block = staged[p, a, :, k * LANES : (k + 1) * LANES].T.reshape(LANES // SUB, SUB, LANES)
                block = block.astype(jnp.bfloat16)
                for i in range(LANES // SUB):
                    g = k * (LANES // SUB) + i
                    send[p, g // tiles, a * tiles + g % tiles] = block[i]
        recv[p, rows] = send[p, rows]

    def move(p, peer):
        return pltpu.make_async_remote_copy(
            send.at[p, peer], recv.at[p, rows], send_sem.at[p], recv_sem.at[p],
            device_id={"rows": peer}, device_id_type=MESH,
        )

    def send_all(p):
        for peer in peers:
            move(p, peer).start()

    def all_of(p):
        others = pl.ds(0, ROWS - 1)
        return pltpu.make_async_remote_copy(
            send.at[p, others], recv.at[p, others], send_sem.at[p], recv_sem.at[p],
            device_id={"rows": rows}, device_id_type=MESH,
        )

    def assemble(p):
        all_of(p).wait_recv()

        def some(t, _):
            for i in range(TOGETHER):
                j = t * TOGETHER + i
                low, high = merged(recv[p, 2 * j], recv[p, 2 * j + 1])
                lanes = pl.ds(pl.multiple_of(j * LANES, LANES), LANES)
                for a, out in enumerate((out_gate, out_up)):
                    out[2 * p, :, :, lanes] = low[a * tiles : (a + 1) * tiles]
                    out[2 * p + 1, :, :, lanes] = high[a * tiles : (a + 1) * tiles]
            return 0

        lax.fori_loop(0, ROWS // 2 // TOGETHER, some, 0)

    def to_z(k):
        mine = pieces.at[core, y, x, z]
        return pltpu.make_async_remote_copy(
            mine, mine, piece_send.at[0], piece_recv.at[0],
            device_id={"rows": beside(z, k, NZ) * NX + x}, device_id_type=MESH,
        )

    def to_x(k):
        mine = pieces.at[core, y, x]
        return pltpu.make_async_remote_copy(
            mine, mine, piece_send.at[1], piece_recv.at[1],
            device_id={"rows": z * NX + beside(x, k, NX)}, device_id_type=MESH,
        )

    def to_y(k):
        mine = pieces.at[core, y]
        return pltpu.make_async_remote_copy(
            mine, mine, piece_send.at[2], piece_recv.at[2],
            device_id={"owner": beside(y, k, NY) * CORES + core}, device_id_type=MESH,
        )

    def to_core(k):
        mine = pieces.at[core]
        return pltpu.make_async_remote_copy(
            mine, mine, piece_send.at[3], piece_recv.at[3],
            device_id={"owner": partner}, device_id_type=MESH,
        )

    stages = ((to_z, NZ), (to_x, NX), (to_y, NY), (to_core, CORES))

    def begin(stage):
        to, count = stages[stage]
        for k in range(1, count):
            to(k).start()

    def end(stage):
        whole = (
            pieces.at[core, y, x, pl.ds(0, NZ - 1)],
            pieces.at[core, y, pl.ds(0, NX - 1)],
            pieces.at[core, pl.ds(0, NY - 1)],
            pieces.at[core],
        )[stage]
        pltpu.make_async_remote_copy(
            whole, whole, piece_send.at[stage], piece_recv.at[stage],
            device_id={"rows": rows}, device_id_type=MESH,
        ).wait()

    def router():
        for zz in range(NZ):
            for half in range(NX // 2):
                blocks = []
                for o in range(NY * CORES):
                    low, high = merged(
                        pieces[o % CORES, o // CORES, 2 * half, zz], pieces[o % CORES, o // CORES, 2 * half + 1, zz]
                    )
                    blocks += [low, high]
                block = jnp.concatenate([b.astype(jnp.float32) for b in blocks], axis=0)
                at = (zz * NX + 2 * half) * LANES // 2
                out_router[at : at + LANES, :] = block.T.astype(jnp.bfloat16)

    prepare(0)
    pl.semaphore_wait(barrier, 2 + (NX - 1) + NY)
    for r, reach in enumerate(REACH):
        if r:
            pl.semaphore_wait(rounds.at[r - 1], 2)
        if r < len(REACH) - 1:
            for peer in beside_z:
                pl.semaphore_signal(rounds.at[r], inc=1, device_id={"rows": peer}, device_id_type=MESH)
        if r == len(REACH) - 2:
            begin(0)
        for p in range(EARLY):
            if r == 0 and p > 0:
                prepare(p)
            for dx, dz in reach:
                move(p, lines[dz] + columns[dx]).start()
    end(0)
    begin(1)
    for p in range(EARLY, 4):
        prepare(p)
        send_all(p)
    end(1)
    begin(2)

    def rest(p, _):
        prepare(p)
        send_all(p)
        return 0

    lax.fori_loop(4, pairs, rest, 0)
    assemble(0)
    end(2)
    begin(3)
    assemble(1)
    end(3)
    router()

    def finish(p, _):
        assemble(p)
        return 0

    lax.fori_loop(2, pairs, finish, 0)

    def sent(p, _):
        all_of(p).wait_send()
        return 0

    lax.fori_loop(0, pairs, sent, 0)


def store(*refs):
    count = len(refs) // 2
    copies = []
    for k, (source, target) in enumerate(zip(refs[:count], refs[count : 2 * count])):
        step = source.shape[0] // PARTS
        for i in range(PARTS):
            part = pl.ds(i * step, step)
            copies.append(pltpu.make_async_copy(source.at[part], target.at[part], refs[-1].at[k, i]))
    for copy in copies:
        copy.start()
    for copy in copies:
        copy.wait()


def pinned(value):
    return pltpu.with_memory_space_constraint(value, pltpu.HBM)


def body(w_gate, w_up, router_weight, router_gain):
    experts, share, width = w_gate.shape
    pairs, model = experts // 2, share * ROWS
    tiles = width // ROWS // SUB
    paired = (pairs, 2 * share, width)
    hbm = pl.BlockSpec(memory_space=pltpu.HBM)
    vmem, anywhere = pl.BlockSpec(memory_space=pltpu.VMEM), pl.BlockSpec(memory_space=pl.ANY)
    gate, up, router = pl.pallas_call(
        kernel,
        out_shape=(
            jax.ShapeDtypeStruct((experts, tiles, SUB, model), jnp.bfloat16),
            jax.ShapeDtypeStruct((experts, tiles, SUB, model), jnp.bfloat16),
            jax.ShapeDtypeStruct((model, experts * NY * CORES), jnp.bfloat16),
        ),
        in_specs=[anywhere, anywhere, hbm, hbm],
        out_specs=(vmem, vmem, vmem),
        scratch_shapes=[
            pltpu.VMEM((pairs, 2, 2 * share, width), jnp.float32),
            pltpu.VMEM((experts, share), jnp.float32),
            pltpu.VMEM((1, share), jnp.float32),
            pltpu.VMEM((pairs, ROWS, 2 * tiles, SUB, LANES), jnp.bfloat16),
            pltpu.VMEM((pairs, ROWS, 2 * tiles, SUB, LANES), jnp.bfloat16),
            pltpu.VMEM((CORES, NY, NX, NZ, SUB, LANES), jnp.bfloat16),
            pltpu.SemaphoreType.DMA((pairs,)),
            pltpu.SemaphoreType.DMA((2,)),
            pltpu.SemaphoreType.DMA((pairs,)),
            pltpu.SemaphoreType.DMA((pairs,)),
            pltpu.SemaphoreType.DMA((4,)),
            pltpu.SemaphoreType.DMA((4,)),
            pltpu.SemaphoreType.REGULAR((len(REACH) - 1,)),
        ],
        compiler_params=pltpu.CompilerParams(collective_id=0, has_side_effects=True, vmem_limit_bytes=50000000),
        name="serve",
    )(w_gate.reshape(paired), w_up.reshape(paired), pinned(router_weight.T), pinned(router_gain.reshape(1, share)))
    gate, up, router = pl.pallas_call(
        store,
        out_shape=tuple(jax.ShapeDtypeStruct(v.shape, v.dtype) for v in (gate, up, router)),
        in_specs=[vmem] * 3,
        out_specs=(anywhere,) * 3,
        scratch_shapes=[pltpu.SemaphoreType.DMA((3, PARTS))],
        compiler_params=pltpu.CompilerParams(vmem_limit_bytes=50000000),
        name="store",
    )(gate, up, router)
    shape = (experts, tiles * SUB, model)
    return gate.reshape(shape), up.reshape(shape), router


def solution(mesh):
    return jax.shard_map(
        body,
        mesh=mesh,
        in_specs=(P("owner", "rows", None), P("owner", "rows", None), P("rows", "owner"), P("rows")),
        out_specs=(P("owner", "rows", None), P("owner", "rows", None), P()),
        check_vma=False,
    )
```

```python
import jax
import jax.numpy as jnp
from jax import lax
from jax.experimental import pallas as pl
from jax.experimental.pallas import tpu as pltpu
from jax.sharding import PartitionSpec as P

MESH = pl.DeviceIdType.MESH
NZ, NX, NY, CORES = 8, 4, 4, 2
ROWS = NZ * NX
LANES, SUB = 128, 8
TOGETHER = 8
PARTS = 4
EARLY = 2
LATE = 2
GROUPS = ((0, 1, 2, 3), (4, 7, 5, 6))
REACH = [
    [(0, dz) for dz in sorted({r + 1, NZ - r - 1}) if r + 1 <= NZ // 2]
    + [(dx, dz) for dz in sorted({r, (NZ - r) % NZ}) for dx in range(1, NX)]
    for r in range(NZ // 2 + 1)
]
ORDER = [(dx, dz) for dx in (2, 1, 3, 0) for dz in (4, 3, 5, 2, 6, 1, 7, 0) if dx or dz]


def place():
    owner, rows = lax.axis_index("owner"), lax.axis_index("rows")
    return owner // CORES, owner % CORES, rows // NX, rows % NX


def beside(value, step, count):
    return (value + step) % count


def merged(even, odd):
    low = lax.broadcasted_iota(jnp.int32, even.shape, even.ndim - 1) < LANES // 2
    turned = pltpu.roll(jnp.where(low, odd, even), LANES // 2, even.ndim - 1)
    return jnp.where(low, even, turned), jnp.where(low, turned, odd)


def kernel(
    gate, up, weight, gain, out_gate, out_up, out_router,
    staged, weights, gains, send, recv, pieces, in_sem, router_sem, send_sem, recv_sem, piece_send, piece_recv, rounds,
):
    y, core, z, x = place()
    owner, rows = lax.axis_index("owner"), lax.axis_index("rows")
    pairs = gate.shape[0]
    width = gate.shape[2]
    tiles = width // ROWS // SUB
    sources = (gate, up)

    def load(a, p):
        return pltpu.make_async_copy(sources[a].at[p], staged.at[p, a], in_sem.at[p])

    def load_all(p, _):
        for a in range(2):
            load(a, p).start()
        return 0

    barrier = pltpu.get_barrier_semaphore()

    lines = [beside(z, dz, NZ) * NX for dz in range(NZ)]
    columns = [beside(x, dx, NX) for dx in range(NX)]
    peers = [lines[dz] + columns[dx] for dx, dz in ORDER]
    y_peers = [beside(y, k, NY) * CORES + core for k in range(1, NY)]
    partner = y * CORES + (1 - core)
    beside_z = [lines[1] + x, lines[NZ - 1] + x]
    for peer in beside_z + [z * NX + columns[dx] for dx in range(1, NX)]:
        pl.semaphore_signal(barrier, inc=1, device_id={"rows": peer}, device_id_type=MESH)
    for peer in (*y_peers, partner):
        pl.semaphore_signal(barrier, inc=1, device_id={"owner": peer}, device_id_type=MESH)

    router_loads = (
        pltpu.make_async_copy(weight, weights, router_sem.at[0]),
        pltpu.make_async_copy(gain, gains, router_sem.at[1]),
    )
    for copy in router_loads:
        copy.start()
    lax.fori_loop(0, pairs, load_all, 0)

    for copy in router_loads:
        copy.wait()
    scaled = weights[...] * gains[...]
    pieces[core, y, x, z] = jnp.concatenate([scaled[:SUB], scaled[SUB:]], axis=1).astype(jnp.bfloat16)

    def prepare(p):
        pltpu.make_async_copy(gate.at[pl.ds(0, 2)], staged.at[p], in_sem.at[p]).wait()
        for a in range(2):
            for k in range(width // LANES):
                block = staged[p, a, :, k * LANES : (k + 1) * LANES].T.reshape(LANES // SUB, SUB, LANES)
                block = block.astype(jnp.bfloat16)
                for i in range(LANES // SUB):
                    g = k * (LANES // SUB) + i
                    send[p, g // tiles, a * tiles + g % tiles] = block[i]
        recv[p, rows] = send[p, rows]

    def move(p, peer):
        return pltpu.make_async_remote_copy(
            send.at[p, peer], recv.at[p, rows], send_sem.at[0], recv_sem.at[p],
            device_id={"rows": peer}, device_id_type=MESH,
        )

    def send_all(p):
        for peer in peers:
            move(p, peer).start()

    def all_of(p):
        others = pl.ds(0, ROWS - 1)
        return pltpu.make_async_remote_copy(
            send.at[p, others], recv.at[p, others], send_sem.at[0], recv_sem.at[p],
            device_id={"rows": rows}, device_id_type=MESH,
        )

    def assemble(p):
        all_of(p).wait_recv()

        def some(t, _):
            for i in range(TOGETHER):
                j = t * TOGETHER + i
                low, high = merged(recv[p, 2 * j], recv[p, 2 * j + 1])
                lanes = pl.ds(pl.multiple_of(j * LANES, LANES), LANES)
                for a, out in enumerate((out_gate, out_up)):
                    out[2 * p, :, :, lanes] = low[a * tiles : (a + 1) * tiles]
                    out[2 * p + 1, :, :, lanes] = high[a * tiles : (a + 1) * tiles]
            return 0

        lax.fori_loop(0, ROWS // 2 // TOGETHER, some, 0)

    def to_z(k):
        mine = pieces.at[core, y, x, z]
        return pltpu.make_async_remote_copy(
            mine, mine, piece_send.at[0], piece_recv.at[0],
            device_id={"rows": beside(z, k, NZ) * NX + x}, device_id_type=MESH,
        )

    def to_x(k):
        mine = pieces.at[core, y, x]
        return pltpu.make_async_remote_copy(
            mine, mine, piece_send.at[1], piece_recv.at[1],
            device_id={"rows": z * NX + beside(x, k, NX)}, device_id_type=MESH,
        )

    def to_y(k):
        mine = pieces.at[core, y]
        return pltpu.make_async_remote_copy(
            mine, mine, piece_send.at[2], piece_recv.at[2],
            device_id={"owner": beside(y, k, NY) * CORES + core}, device_id_type=MESH,
        )

    def to_core(k):
        mine = pieces.at[core]
        return pltpu.make_async_remote_copy(
            mine, mine, piece_send.at[3], piece_recv.at[3],
            device_id={"owner": partner}, device_id_type=MESH,
        )

    stages = ((to_z, NZ), (to_x, NX), (to_y, NY), (to_core, CORES))

    def begin(stage):
        to, count = stages[stage]
        for k in range(1, count):
            to(k).start()

    def end(stage):
        whole = (
            pieces.at[core, y, x, pl.ds(0, NZ - 1)],
            pieces.at[core, y, pl.ds(0, NX - 1)],
            pieces.at[core, pl.ds(0, NY - 1)],
            pieces.at[core],
        )[stage]
        pltpu.make_async_remote_copy(
            whole, whole, piece_send.at[stage], piece_recv.at[stage],
            device_id={"rows": rows}, device_id_type=MESH,
        ).wait()

    def router():
        for zz in range(NZ):
            for half in range(NX // 2):
                blocks = []
                for o in range(NY * CORES):
                    low, high = merged(
                        pieces[o % CORES, o // CORES, 2 * half, zz], pieces[o % CORES, o // CORES, 2 * half + 1, zz]
                    )
                    blocks += [low, high]
                block = jnp.concatenate([b.astype(jnp.float32) for b in blocks], axis=0)
                at = (zz * NX + 2 * half) * LANES // 2
                out_router[at : at + LANES, :] = block.T.astype(jnp.bfloat16)

    prepare(0)
    pl.semaphore_wait(barrier, 2 + (NX - 1) + NY)
    for r, reach in enumerate(REACH):
        if r:
            pl.semaphore_wait(rounds.at[r - 1], 2)
        if r < len(REACH) - 1:
            for peer in beside_z:
                pl.semaphore_signal(rounds.at[r], inc=1, device_id={"rows": peer}, device_id_type=MESH)
        if r == len(REACH) - 2:
            begin(0)
        for p in range(EARLY):
            if r == 0 and p > 0:
                prepare(p)
            for dx, dz in reach:
                move(p, lines[dz] + columns[dx]).start()
    end(0)
    begin(1)
    for p in range(EARLY, 4):
        prepare(p)
        send_all(p)
    end(1)
    begin(2)

    def rest(p, _):
        prepare(p)
        send_all(p)
        return 0

    lax.fori_loop(4, pairs - LATE, rest, 0)
    for p in range(pairs - LATE, pairs):
        prepare(p)
    for group in GROUPS:
        for column in columns[2], columns[1], columns[3], x:
            for line in group:
                for p in range(pairs - LATE, pairs):

                    @pl.when(line * NX + column != rows)
                    def _():
                        move(p, line * NX + column).start()

    assemble(0)
    end(2)
    begin(3)
    assemble(1)
    end(3)
    router()

    def finish(p, _):
        assemble(p)
        return 0

    lax.fori_loop(2, pairs, finish, 0)

    others = pl.ds(0, ROWS - 1)
    pltpu.make_async_remote_copy(
        send.at[:, others], recv.at[:, others], send_sem.at[0], recv_sem.at[0],
        device_id={"rows": rows}, device_id_type=MESH,
    ).wait_send()


def store(*refs):
    count = len(refs) // 2
    copies = []
    for k, (source, target) in enumerate(zip(refs[:count], refs[count : 2 * count])):
        step = source.shape[0] // PARTS
        for i in range(PARTS):
            part = pl.ds(i * step, step)
            copies.append(pltpu.make_async_copy(source.at[part], target.at[part], refs[-1].at[k]))
    for copy in copies:
        copy.start()
    for k, (source, target) in enumerate(zip(refs[:count], refs[count : 2 * count])):
        pltpu.make_async_copy(source, target, refs[-1].at[k]).wait()


def pinned(value):
    return pltpu.with_memory_space_constraint(value, pltpu.HBM)


def body(w_gate, w_up, router_weight, router_gain):
    experts, share, width = w_gate.shape
    pairs, model = experts // 2, share * ROWS
    tiles = width // ROWS // SUB
    paired = (pairs, 2 * share, width)
    hbm = pl.BlockSpec(memory_space=pltpu.HBM)
    vmem, anywhere = pl.BlockSpec(memory_space=pltpu.VMEM), pl.BlockSpec(memory_space=pl.ANY)
    gate, up, router = pl.pallas_call(
        kernel,
        out_shape=(
            jax.ShapeDtypeStruct((experts, tiles, SUB, model), jnp.bfloat16),
            jax.ShapeDtypeStruct((experts, tiles, SUB, model), jnp.bfloat16),
            jax.ShapeDtypeStruct((model, experts * NY * CORES), jnp.bfloat16),
        ),
        in_specs=[anywhere, anywhere, hbm, hbm],
        out_specs=(vmem, vmem, vmem),
        scratch_shapes=[
            pltpu.VMEM((pairs, 2, 2 * share, width), jnp.float32),
            pltpu.VMEM((experts, share), jnp.float32),
            pltpu.VMEM((1, share), jnp.float32),
            pltpu.VMEM((pairs, ROWS, 2 * tiles, SUB, LANES), jnp.bfloat16),
            pltpu.VMEM((pairs, ROWS, 2 * tiles, SUB, LANES), jnp.bfloat16),
            pltpu.VMEM((CORES, NY, NX, NZ, SUB, LANES), jnp.bfloat16),
            pltpu.SemaphoreType.DMA((pairs,)),
            pltpu.SemaphoreType.DMA((2,)),
            pltpu.SemaphoreType.DMA((1,)),
            pltpu.SemaphoreType.DMA((pairs,)),
            pltpu.SemaphoreType.DMA((4,)),
            pltpu.SemaphoreType.DMA((4,)),
            pltpu.SemaphoreType.REGULAR((len(REACH) - 1,)),
        ],
        compiler_params=pltpu.CompilerParams(collective_id=0, has_side_effects=True, vmem_limit_bytes=50000000),
        name="serve",
    )(w_gate.reshape(paired), w_up.reshape(paired), pinned(router_weight.T), pinned(router_gain.reshape(1, share)))
    gate, up, router = pl.pallas_call(
        store,
        out_shape=tuple(jax.ShapeDtypeStruct(v.shape, v.dtype) for v in (gate, up, router)),
        in_specs=[vmem] * 3,
        out_specs=(anywhere,) * 3,
        scratch_shapes=[pltpu.SemaphoreType.DMA((3,))],
        compiler_params=pltpu.CompilerParams(vmem_limit_bytes=50000000),
        name="store",
    )(gate, up, router)
    shape = (experts, tiles * SUB, model)
    return gate.reshape(shape), up.reshape(shape), router


def solution(mesh):
    return jax.shard_map(
        body,
        mesh=mesh,
        in_specs=(P("owner", "rows", None), P("owner", "rows", None), P("rows", "owner"), P("rows")),
        out_specs=(P("owner", "rows", None), P("owner", "rows", None), P()),
        check_vma=False,
    )
```

```python
import jax
import jax.numpy as jnp
from jax import lax
from jax.experimental import pallas as pl
from jax.experimental.pallas import tpu as pltpu
from jax.sharding import PartitionSpec as P

MESH = pl.DeviceIdType.MESH
NZ, NX, NY, CORES = 8, 4, 4, 2
ROWS = NZ * NX
LANES, SUB = 128, 8
TOGETHER = 16
PARTS = 4
EARLY = 2
LATE = 4
GROUPS = ((0, 1, 2, 3), (7, 4, 6, 5))
REACH = [
    [(0, dz) for dz in sorted({r + 1, NZ - r - 1}) if r + 1 <= NZ // 2]
    + [(dx, dz) for dz in sorted({r, (NZ - r) % NZ}) for dx in range(1, NX)]
    for r in range(NZ // 2 + 1)
]
ORDER = [(dx, dz) for dx in (2, 1, 3, 0) for dz in (4, 3, 5, 2, 6, 1, 7, 0) if dx or dz]


def place():
    owner, rows = lax.axis_index("owner"), lax.axis_index("rows")
    return owner // CORES, owner % CORES, rows // NX, rows % NX


def beside(value, step, count):
    return (value + step) % count


def merged(even, odd):
    low = lax.broadcasted_iota(jnp.int32, even.shape, even.ndim - 1) < LANES // 2
    turned = pltpu.roll(jnp.where(low, odd, even), LANES // 2, even.ndim - 1)
    return jnp.where(low, even, turned), jnp.where(low, turned, odd)


def kernel(
    gate, up, weight, gain, out_gate, out_up, out_router,
    staged, weights, gains, send, recv, pieces, in_sem, router_sem, send_sem, recv_sem, piece_send, piece_recv, rounds,
):
    y, core, z, x = place()
    owner, rows = lax.axis_index("owner"), lax.axis_index("rows")
    pairs = gate.shape[0]
    width = gate.shape[2]
    tiles = width // ROWS // SUB
    sources = (gate, up)

    def load(a, p):
        return pltpu.make_async_copy(sources[a].at[p], staged.at[p, a], in_sem.at[p])

    def load_all(p, _):
        for a in range(2):
            load(a, p).start()
        return 0

    barrier = pltpu.get_barrier_semaphore()

    lines = [beside(z, dz, NZ) * NX for dz in range(NZ)]
    columns = [beside(x, dx, NX) for dx in range(NX)]
    peers = [lines[dz] + columns[dx] for dx, dz in ORDER]
    y_peers = [beside(y, k, NY) * CORES + core for k in range(1, NY)]
    partner = y * CORES + (1 - core)
    beside_z = [lines[1] + x, lines[NZ - 1] + x]
    for peer in beside_z + [z * NX + columns[dx] for dx in range(1, NX)]:
        pl.semaphore_signal(barrier, inc=1, device_id={"rows": peer}, device_id_type=MESH)
    for peer in (*y_peers, partner):
        pl.semaphore_signal(barrier, inc=1, device_id={"owner": peer}, device_id_type=MESH)

    router_loads = (
        pltpu.make_async_copy(weight, weights, router_sem.at[0]),
        pltpu.make_async_copy(gain, gains, router_sem.at[1]),
    )
    for copy in router_loads:
        copy.start()
    lax.fori_loop(0, pairs, load_all, 0)

    for copy in router_loads:
        copy.wait()
    scaled = weights[...] * gains[...]
    pieces[core, y, x, z] = jnp.concatenate([scaled[:SUB], scaled[SUB:]], axis=1).astype(jnp.bfloat16)

    def prepare(p):
        pltpu.make_async_copy(gate.at[pl.ds(0, 2)], staged.at[p], in_sem.at[p]).wait()
        for a in range(2):
            for k in range(width // LANES):
                block = staged[p, a, :, k * LANES : (k + 1) * LANES].T.reshape(LANES // SUB, SUB, LANES)
                block = block.astype(jnp.bfloat16)
                for i in range(LANES // SUB):
                    g = k * (LANES // SUB) + i
                    send[p, g // tiles, a * tiles + g % tiles] = block[i]
        recv[p, rows] = send[p, rows]

    def move(p, peer):
        return pltpu.make_async_remote_copy(
            send.at[p, peer], recv.at[p, rows], send_sem.at[0], recv_sem.at[p],
            device_id={"rows": peer}, device_id_type=MESH,
        )

    def send_all(p):
        for peer in peers:
            move(p, peer).start()

    def all_of(p):
        others = pl.ds(0, ROWS - 1)
        return pltpu.make_async_remote_copy(
            send.at[p, others], recv.at[p, others], send_sem.at[0], recv_sem.at[p],
            device_id={"rows": rows}, device_id_type=MESH,
        )

    def assemble(p):
        all_of(p).wait_recv()

        def some(t, _):
            for i in range(TOGETHER):
                j = t * TOGETHER + i
                low, high = merged(recv[p, 2 * j], recv[p, 2 * j + 1])
                lanes = pl.ds(pl.multiple_of(j * LANES, LANES), LANES)
                for a, out in enumerate((out_gate, out_up)):
                    out[2 * p, :, :, lanes] = low[a * tiles : (a + 1) * tiles]
                    out[2 * p + 1, :, :, lanes] = high[a * tiles : (a + 1) * tiles]
            return 0

        lax.fori_loop(0, ROWS // 2 // TOGETHER, some, 0)

    def to_z(k):
        mine = pieces.at[core, y, x, z]
        return pltpu.make_async_remote_copy(
            mine, mine, piece_send.at[0], piece_recv.at[0],
            device_id={"rows": beside(z, k, NZ) * NX + x}, device_id_type=MESH,
        )

    def to_x(k):
        mine = pieces.at[core, y, x]
        return pltpu.make_async_remote_copy(
            mine, mine, piece_send.at[1], piece_recv.at[1],
            device_id={"rows": z * NX + beside(x, k, NX)}, device_id_type=MESH,
        )

    def to_y(k):
        mine = pieces.at[core, y]
        return pltpu.make_async_remote_copy(
            mine, mine, piece_send.at[2], piece_recv.at[2],
            device_id={"owner": beside(y, k, NY) * CORES + core}, device_id_type=MESH,
        )

    def to_core(k):
        mine = pieces.at[core]
        return pltpu.make_async_remote_copy(
            mine, mine, piece_send.at[3], piece_recv.at[3],
            device_id={"owner": partner}, device_id_type=MESH,
        )

    stages = ((to_z, NZ), (to_x, NX), (to_y, NY), (to_core, CORES))

    def begin(stage):
        to, count = stages[stage]
        for k in range(1, count):
            to(k).start()

    def end(stage):
        whole = (
            pieces.at[core, y, x, pl.ds(0, NZ - 1)],
            pieces.at[core, y, pl.ds(0, NX - 1)],
            pieces.at[core, pl.ds(0, NY - 1)],
            pieces.at[core],
        )[stage]
        pltpu.make_async_remote_copy(
            whole, whole, piece_send.at[stage], piece_recv.at[stage],
            device_id={"rows": rows}, device_id_type=MESH,
        ).wait()

    def router():
        for zz in range(NZ):
            for half in range(NX // 2):
                blocks = []
                for o in range(NY * CORES):
                    low, high = merged(
                        pieces[o % CORES, o // CORES, 2 * half, zz], pieces[o % CORES, o // CORES, 2 * half + 1, zz]
                    )
                    blocks += [low, high]
                block = jnp.concatenate([b.astype(jnp.float32) for b in blocks], axis=0)
                at = (zz * NX + 2 * half) * LANES // 2
                out_router[at : at + LANES, :] = block.T.astype(jnp.bfloat16)

    prepare(0)
    pl.semaphore_wait(barrier, 2 + (NX - 1) + NY)
    for r, reach in enumerate(REACH):
        if r:
            pl.semaphore_wait(rounds.at[r - 1], 2)
        if r < len(REACH) - 1:
            for peer in beside_z:
                pl.semaphore_signal(rounds.at[r], inc=1, device_id={"rows": peer}, device_id_type=MESH)
        if r == len(REACH) - 2:
            begin(0)
        for p in range(EARLY):
            if r == 0 and p > 0:
                prepare(p)
            for dx, dz in reach:
                move(p, lines[dz] + columns[dx]).start()
    end(0)
    begin(1)
    for p in range(EARLY, 4):
        prepare(p)
        send_all(p)
    end(1)
    begin(2)

    def rest(p, _):
        prepare(p)
        send_all(p)
        return 0

    lax.fori_loop(4, pairs - LATE, rest, 0)
    for p in range(pairs - LATE, pairs):
        prepare(p)
    for group in GROUPS:
        for column in columns[2], columns[1], columns[3], x:
            for line in group:
                late = (line + NZ // 2 * core) % NZ * NX + column
                for p in range(pairs - LATE, pairs):

                    @pl.when(late != rows)
                    def _():
                        move(p, late).start()

    assemble(0)
    end(2)
    begin(3)
    assemble(1)
    end(3)
    router()

    def finish(p, _):
        assemble(p)
        return 0

    lax.fori_loop(2, pairs, finish, 0)

    others = pl.ds(0, ROWS - 1)
    pltpu.make_async_remote_copy(
        send.at[:, others], recv.at[:, others], send_sem.at[0], recv_sem.at[0],
        device_id={"rows": rows}, device_id_type=MESH,
    ).wait_send()


def store(*refs):
    count = len(refs) // 2
    copies = []
    for k, (source, target) in enumerate(zip(refs[:count], refs[count : 2 * count])):
        step = source.shape[0] // PARTS
        for i in range(PARTS):
            part = pl.ds(i * step, step)
            copies.append(pltpu.make_async_copy(source.at[part], target.at[part], refs[-1].at[k]))
    for copy in copies:
        copy.start()
    for k, (source, target) in enumerate(zip(refs[:count], refs[count : 2 * count])):
        pltpu.make_async_copy(source, target, refs[-1].at[k]).wait()


def pinned(value):
    return pltpu.with_memory_space_constraint(value, pltpu.HBM)


def body(w_gate, w_up, router_weight, router_gain):
    experts, share, width = w_gate.shape
    pairs, model = experts // 2, share * ROWS
    tiles = width // ROWS // SUB
    paired = (pairs, 2 * share, width)
    hbm = pl.BlockSpec(memory_space=pltpu.HBM)
    vmem, anywhere = pl.BlockSpec(memory_space=pltpu.VMEM), pl.BlockSpec(memory_space=pl.ANY)
    gate, up, router = pl.pallas_call(
        kernel,
        out_shape=(
            jax.ShapeDtypeStruct((experts, tiles, SUB, model), jnp.bfloat16),
            jax.ShapeDtypeStruct((experts, tiles, SUB, model), jnp.bfloat16),
            jax.ShapeDtypeStruct((model, experts * NY * CORES), jnp.bfloat16),
        ),
        in_specs=[anywhere, anywhere, hbm, hbm],
        out_specs=(vmem, vmem, vmem),
        scratch_shapes=[
            pltpu.VMEM((pairs, 2, 2 * share, width), jnp.float32),
            pltpu.VMEM((experts, share), jnp.float32),
            pltpu.VMEM((1, share), jnp.float32),
            pltpu.VMEM((pairs, ROWS, 2 * tiles, SUB, LANES), jnp.bfloat16),
            pltpu.VMEM((pairs, ROWS, 2 * tiles, SUB, LANES), jnp.bfloat16),
            pltpu.VMEM((CORES, NY, NX, NZ, SUB, LANES), jnp.bfloat16),
            pltpu.SemaphoreType.DMA((pairs,)),
            pltpu.SemaphoreType.DMA((2,)),
            pltpu.SemaphoreType.DMA((1,)),
            pltpu.SemaphoreType.DMA((pairs,)),
            pltpu.SemaphoreType.DMA((4,)),
            pltpu.SemaphoreType.DMA((4,)),
            pltpu.SemaphoreType.REGULAR((len(REACH) - 1,)),
        ],
        compiler_params=pltpu.CompilerParams(collective_id=0, has_side_effects=True, vmem_limit_bytes=50000000),
        name="serve",
    )(w_gate.reshape(paired), w_up.reshape(paired), pinned(router_weight.T), pinned(router_gain.reshape(1, share)))
    gate, up, router = pl.pallas_call(
        store,
        out_shape=tuple(jax.ShapeDtypeStruct(v.shape, v.dtype) for v in (gate, up, router)),
        in_specs=[vmem] * 3,
        out_specs=(anywhere,) * 3,
        scratch_shapes=[pltpu.SemaphoreType.DMA((3,))],
        compiler_params=pltpu.CompilerParams(vmem_limit_bytes=50000000),
        name="store",
    )(gate, up, router)
    shape = (experts, tiles * SUB, model)
    return gate.reshape(shape), up.reshape(shape), router


def solution(mesh):
    return jax.shard_map(
        body,
        mesh=mesh,
        in_specs=(P("owner", "rows", None), P("owner", "rows", None), P("rows", "owner"), P("rows")),
        out_specs=(P("owner", "rows", None), P("owner", "rows", None), P()),
        check_vma=False,
    )
```

```python
import jax
import jax.numpy as jnp
from jax import lax
from jax.experimental import pallas as pl
from jax.experimental.pallas import tpu as pltpu
from jax.sharding import PartitionSpec as P

MESH = pl.DeviceIdType.MESH
NZ, NX, NY, CORES = 8, 4, 4, 2
ROWS = NZ * NX
LANES, SUB = 128, 8
TOGETHER = 16
PARTS = 4
EARLY = 2
LATE = 5
GROUPS = ((0, 1, 2, 3), (7, 4, 6, 5))
REACH = [
    [(0, dz) for dz in sorted({r + 1, NZ - r - 1}) if r + 1 <= NZ // 2]
    + [(dx, dz) for dz in sorted({r, (NZ - r) % NZ}) for dx in range(1, NX)]
    for r in range(NZ // 2 + 1)
]
ORDER = [(dx, dz) for dx in (2, 1, 3, 0) for dz in (4, 3, 5, 2, 6, 1, 7, 0) if dx or dz]


def place():
    owner, rows = lax.axis_index("owner"), lax.axis_index("rows")
    return owner // CORES, owner % CORES, rows // NX, rows % NX


def beside(value, step, count):
    return (value + step) % count


def merged(even, odd):
    low = lax.broadcasted_iota(jnp.int32, even.shape, even.ndim - 1) < LANES // 2
    turned = pltpu.roll(jnp.where(low, odd, even), LANES // 2, even.ndim - 1)
    return jnp.where(low, even, turned), jnp.where(low, turned, odd)


def kernel(
    gate, up, weight, gain, out_gate, out_up, out_router,
    staged, weights, gains, send, recv, pieces, in_sem, router_sem, send_sem, recv_sem, piece_send, piece_recv, rounds,
):
    y, core, z, x = place()
    owner, rows = lax.axis_index("owner"), lax.axis_index("rows")
    pairs = gate.shape[0]
    width = gate.shape[2]
    tiles = width // ROWS // SUB
    sources = (gate, up)

    def load(a, p):
        return pltpu.make_async_copy(sources[a].at[p], staged.at[p, a], in_sem.at[p])

    def load_all(p, _):
        for a in range(2):
            load(a, p).start()
        return 0

    barrier = pltpu.get_barrier_semaphore()

    lines = [beside(z, dz, NZ) * NX for dz in range(NZ)]
    columns = [beside(x, dx, NX) for dx in range(NX)]
    peers = [lines[dz] + columns[dx] for dx, dz in ORDER]
    y_peers = [beside(y, k, NY) * CORES + core for k in range(1, NY)]
    partner = y * CORES + (1 - core)
    beside_z = [lines[1] + x, lines[NZ - 1] + x]
    for peer in beside_z + [z * NX + columns[dx] for dx in range(1, NX)]:
        pl.semaphore_signal(barrier, inc=1, device_id={"rows": peer}, device_id_type=MESH)
    for peer in (*y_peers, partner):
        pl.semaphore_signal(barrier, inc=1, device_id={"owner": peer}, device_id_type=MESH)

    router_loads = (
        pltpu.make_async_copy(weight, weights, router_sem.at[0]),
        pltpu.make_async_copy(gain, gains, router_sem.at[1]),
    )
    for copy in router_loads:
        copy.start()
    lax.fori_loop(0, pairs, load_all, 0)

    for copy in router_loads:
        copy.wait()
    scaled = weights[...] * gains[...]
    pieces[core, y, x, z] = jnp.concatenate([scaled[:SUB], scaled[SUB:]], axis=1).astype(jnp.bfloat16)

    def prepare(p):
        pltpu.make_async_copy(gate.at[pl.ds(0, 2)], staged.at[p], in_sem.at[p]).wait()
        for a in range(2):
            for k in range(width // LANES):
                block = staged[p, a, :, k * LANES : (k + 1) * LANES].T.reshape(LANES // SUB, SUB, LANES)
                block = block.astype(jnp.bfloat16)
                for i in range(LANES // SUB):
                    g = k * (LANES // SUB) + i
                    send[p, g // tiles, a * tiles + g % tiles] = block[i]
        recv[p, rows] = send[p, rows]

    def move(p, peer):
        return pltpu.make_async_remote_copy(
            send.at[p, peer], recv.at[p, rows], send_sem.at[0], recv_sem.at[p],
            device_id={"rows": peer}, device_id_type=MESH,
        )

    def send_all(p):
        for peer in peers:
            move(p, peer).start()

    def all_of(p):
        others = pl.ds(0, ROWS - 1)
        return pltpu.make_async_remote_copy(
            send.at[p, others], recv.at[p, others], send_sem.at[0], recv_sem.at[p],
            device_id={"rows": rows}, device_id_type=MESH,
        )

    def assemble(p):
        all_of(p).wait_recv()

        def some(t, _):
            for i in range(TOGETHER):
                j = t * TOGETHER + i
                low, high = merged(recv[p, 2 * j], recv[p, 2 * j + 1])
                lanes = pl.ds(pl.multiple_of(j * LANES, LANES), LANES)
                for a, out in enumerate((out_gate, out_up)):
                    out[2 * p, :, :, lanes] = low[a * tiles : (a + 1) * tiles]
                    out[2 * p + 1, :, :, lanes] = high[a * tiles : (a + 1) * tiles]
            return 0

        lax.fori_loop(0, ROWS // 2 // TOGETHER, some, 0)

    def to_z(k):
        mine = pieces.at[core, y, x, z]
        return pltpu.make_async_remote_copy(
            mine, mine, piece_send.at[0], piece_recv.at[0],
            device_id={"rows": beside(z, k, NZ) * NX + x}, device_id_type=MESH,
        )

    def to_x(k):
        mine = pieces.at[core, y, x]
        return pltpu.make_async_remote_copy(
            mine, mine, piece_send.at[1], piece_recv.at[1],
            device_id={"rows": z * NX + beside(x, k, NX)}, device_id_type=MESH,
        )

    def to_y(k):
        mine = pieces.at[core, y]
        return pltpu.make_async_remote_copy(
            mine, mine, piece_send.at[2], piece_recv.at[2],
            device_id={"owner": beside(y, k, NY) * CORES + core}, device_id_type=MESH,
        )

    def to_core(k):
        mine = pieces.at[core]
        return pltpu.make_async_remote_copy(
            mine, mine, piece_send.at[3], piece_recv.at[3],
            device_id={"owner": partner}, device_id_type=MESH,
        )

    stages = ((to_z, NZ), (to_x, NX), (to_y, NY), (to_core, CORES))

    def begin(stage):
        to, count = stages[stage]
        for k in range(1, count):
            to(k).start()

    def end(stage):
        whole = (
            pieces.at[core, y, x, pl.ds(0, NZ - 1)],
            pieces.at[core, y, pl.ds(0, NX - 1)],
            pieces.at[core, pl.ds(0, NY - 1)],
            pieces.at[core],
        )[stage]
        pltpu.make_async_remote_copy(
            whole, whole, piece_send.at[stage], piece_recv.at[stage],
            device_id={"rows": rows}, device_id_type=MESH,
        ).wait()

    def router():
        for zz in range(NZ):
            for half in range(NX // 2):
                blocks = []
                for o in range(NY * CORES):
                    low, high = merged(
                        pieces[o % CORES, o // CORES, 2 * half, zz], pieces[o % CORES, o // CORES, 2 * half + 1, zz]
                    )
                    blocks += [low, high]
                block = jnp.concatenate([b.astype(jnp.float32) for b in blocks], axis=0)
                at = (zz * NX + 2 * half) * LANES // 2
                out_router[at : at + LANES, :] = block.T.astype(jnp.bfloat16)

    prepare(0)
    pl.semaphore_wait(barrier, 2 + (NX - 1) + NY)
    for r, reach in enumerate(REACH):
        if r:
            pl.semaphore_wait(rounds.at[r - 1], 2)
        if r < len(REACH) - 1:
            for peer in beside_z:
                pl.semaphore_signal(rounds.at[r], inc=1, device_id={"rows": peer}, device_id_type=MESH)
        if r == len(REACH) - 2:
            begin(0)
        for p in range(EARLY):
            if r == 0 and p > 0:
                prepare(p)
            for dx, dz in reach:
                move(p, lines[dz] + columns[dx]).start()
    end(0)
    begin(1)
    for p in range(EARLY, pairs - LATE):
        prepare(p)
        send_all(p)
    end(1)
    begin(2)

    def rest(p, _):
        prepare(p)
        send_all(p)
        return 0

    lax.fori_loop(pairs - LATE, pairs - LATE, rest, 0)
    for p in range(pairs - LATE, pairs):
        prepare(p)
    for group in GROUPS:
        for column in columns[2], columns[1], columns[3], x:
            for line in group:
                late = (line + NZ // 2 * core) % NZ * NX + column
                for p in range(pairs - LATE, pairs):

                    @pl.when(late != rows)
                    def _():
                        move(p, late).start()

    assemble(0)
    end(2)
    begin(3)
    assemble(1)
    end(3)
    router()

    def finish(p, _):
        assemble(p)
        return 0

    lax.fori_loop(2, pairs, finish, 0)

    others = pl.ds(0, ROWS - 1)
    pltpu.make_async_remote_copy(
        send.at[:, others], recv.at[:, others], send_sem.at[0], recv_sem.at[0],
        device_id={"rows": rows}, device_id_type=MESH,
    ).wait_send()


def store(*refs):
    count = len(refs) // 2
    copies = []
    for k, (source, target) in enumerate(zip(refs[:count], refs[count : 2 * count])):
        step = source.shape[0] // PARTS
        for i in range(PARTS):
            part = pl.ds(i * step, step)
            copies.append(pltpu.make_async_copy(source.at[part], target.at[part], refs[-1].at[k]))
    for copy in copies:
        copy.start()
    for k, (source, target) in enumerate(zip(refs[:count], refs[count : 2 * count])):
        pltpu.make_async_copy(source, target, refs[-1].at[k]).wait()


def pinned(value):
    return pltpu.with_memory_space_constraint(value, pltpu.HBM)


def body(w_gate, w_up, router_weight, router_gain):
    experts, share, width = w_gate.shape
    pairs, model = experts // 2, share * ROWS
    tiles = width // ROWS // SUB
    paired = (pairs, 2 * share, width)
    hbm = pl.BlockSpec(memory_space=pltpu.HBM)
    vmem, anywhere = pl.BlockSpec(memory_space=pltpu.VMEM), pl.BlockSpec(memory_space=pl.ANY)
    gate, up, router = pl.pallas_call(
        kernel,
        out_shape=(
            jax.ShapeDtypeStruct((experts, tiles, SUB, model), jnp.bfloat16),
            jax.ShapeDtypeStruct((experts, tiles, SUB, model), jnp.bfloat16),
            jax.ShapeDtypeStruct((model, experts * NY * CORES), jnp.bfloat16),
        ),
        in_specs=[anywhere, anywhere, hbm, hbm],
        out_specs=(vmem, vmem, vmem),
        scratch_shapes=[
            pltpu.VMEM((pairs, 2, 2 * share, width), jnp.float32),
            pltpu.VMEM((experts, share), jnp.float32),
            pltpu.VMEM((1, share), jnp.float32),
            pltpu.VMEM((pairs, ROWS, 2 * tiles, SUB, LANES), jnp.bfloat16),
            pltpu.VMEM((pairs, ROWS, 2 * tiles, SUB, LANES), jnp.bfloat16),
            pltpu.VMEM((CORES, NY, NX, NZ, SUB, LANES), jnp.bfloat16),
            pltpu.SemaphoreType.DMA((pairs,)),
            pltpu.SemaphoreType.DMA((2,)),
            pltpu.SemaphoreType.DMA((1,)),
            pltpu.SemaphoreType.DMA((pairs,)),
            pltpu.SemaphoreType.DMA((4,)),
            pltpu.SemaphoreType.DMA((4,)),
            pltpu.SemaphoreType.REGULAR((len(REACH) - 1,)),
        ],
        compiler_params=pltpu.CompilerParams(collective_id=0, has_side_effects=True, vmem_limit_bytes=50000000),
        name="serve",
    )(w_gate.reshape(paired), w_up.reshape(paired), pinned(router_weight.T), pinned(router_gain.reshape(1, share)))
    gate, up, router = pl.pallas_call(
        store,
        out_shape=tuple(jax.ShapeDtypeStruct(v.shape, v.dtype) for v in (gate, up, router)),
        in_specs=[vmem] * 3,
        out_specs=(anywhere,) * 3,
        scratch_shapes=[pltpu.SemaphoreType.DMA((3,))],
        compiler_params=pltpu.CompilerParams(vmem_limit_bytes=50000000),
        name="store",
    )(gate, up, router)
    shape = (experts, tiles * SUB, model)
    return gate.reshape(shape), up.reshape(shape), router


def solution(mesh):
    return jax.shard_map(
        body,
        mesh=mesh,
        in_specs=(P("owner", "rows", None), P("owner", "rows", None), P("rows", "owner"), P("rows")),
        out_specs=(P("owner", "rows", None), P("owner", "rows", None), P()),
        check_vma=False,
    )
```
